32 devices in a mesh: row: 4 (over z), col: 8 (over y, x, core).
Axes of the slice: x: 2, y: 2, z: 4, core: 2. Of those that a mesh axis runs over, the one named last changes fastest.
Arguments:
- neighbor: int32 [32, 3072, 3072], P(None, 'col', 'row'), may hold values from 0 to 1, as said below
- true_coords: float32 [32, 3, 3072], P(None, None, ('row', 'col')), as said below
- pred_coords: float32 [32, 3, 3072], P(None, None, ('row', 'col')), as said below
- residue_mask: int32 [32, 3072], P(None, ('row', 'col')), may hold values from 0 to 1, as said below
- single: bfloat16 [32, 3072, 384], P(None, ('row', 'col'))
- ln_gain: float32 [384], replicated, may hold values from 0.1 to 1.9
- w_hidden: bfloat16 [384, 128], replicated, may hold values from -0.3125 to 0.3125
- b_hidden: float32 [128], replicated, may hold values from -3 to 3
- w_mid: bfloat16 [128, 128], replicated, may hold values from -0.5 to 0.5
- b_mid: float32 [128], replicated, may hold values from -3 to 3
- w_logits: bfloat16 [128, 50], replicated, may hold values from -1.5 to 1.5
- b_logits: float32 [50], replicated, may hold values from -4 to 4
Outputs:
- lddt_score: float32 [32, 3072], P(None, ('row', 'col'))
- residue_loss: float32 [32, 3072], P(None, ('row', 'col'))
- total_loss: float32 [], replicated
The draws below stay inside these ranges and needn't reach their ends.
Inputs may be any that keep to these rules, and one draw needn't show every extreme that they name: `neighbor`: 0 or 1; 0 where j == i; 1 wherever 0 < |i - j| <= 8. `residue_mask`: per structure, 1 on a leading run of 1536 or more residues and 0 after it. `true_coords`: positions in angstroms. `pred_coords`: positions in angstroms.
All inputs are finite; a program needn't handle non-finite values.
Results may differ from the reference program's by a relative error of at most 0.00098.
Values sent between devices are 32-bit elements; how exact they have to be, the bound alone decides.
A program may use at most 128 MiB of HBM per device.

```python
import math
import jax
import jax.numpy as jnp
from jax import lax

L = 3072
BATCH = 32
C_S = 384
HEAD_WIDTH = 128
BINS = 50


def chain_pair(key):
    base = jax.random.fold_in(key, 7)
    k_step, k_scale, k_noise = jax.random.split(base, 3)
    steps = jax.random.normal(k_step, (BATCH, 3, L), jnp.float32) * 2.2
    truth = jnp.cumsum(steps, axis=2)
    scale = jnp.exp(jax.random.uniform(k_scale, (BATCH, 1, L), jnp.float32, math.log(0.3), math.log(6.0)))
    noise = jax.random.normal(k_noise, (BATCH, 3, L), jnp.float32)
    return (truth, truth + scale * noise)


def draw_true_coords(key, part):
    return chain_pair(key)[0]


def draw_pred_coords(key, part):
    return chain_pair(key)[1]


def draw_neighbor(key, part):
    base = jax.random.fold_in(key, 13)
    rows_index = jnp.arange(L)[:, None]
    cols_index = jnp.arange(L)[None, :]
    apart = jnp.abs(rows_index - cols_index)
    banded = (apart <= 8) & (apart > 0)
    chosen = jax.random.randint(base, (BATCH, L, L), 0, 48) == 0
    linked = (banded[None] | chosen) & (apart > 0)[None]
    return jnp.where(linked, 1, 0).astype(jnp.int32)


def draw_residue_mask(key, part):
    base = jax.random.fold_in(key, 17)
    lengths = jax.random.randint(base, (BATCH, 1), L // 2, L + 1)
    positions = jnp.arange(L)[None, :]
    return jnp.where(positions < lengths, 1, 0).astype(jnp.int32)


def draw_single(key, part):
    base = jax.random.fold_in(key, 3)
    k_value = jax.random.fold_in(base, 0)
    values = jax.random.normal(k_value, (BATCH, L, C_S), jnp.float32)
    return values.astype(jnp.bfloat16)


def normal_values(own_key, extent, width, most, dtype=jnp.bfloat16):
    drawn = width * jax.random.normal(own_key, extent, jnp.float32)
    return jnp.clip(drawn, min=-most, max=most).astype(dtype)


def setup_inputs(seed: int = 0) -> dict:
    arg_keys = jax.random.split(jax.random.key(seed), 13)
    return {
        "neighbor": draw_neighbor(jax.random.fold_in(arg_keys[12], 71), 0),
        "true_coords": draw_true_coords(jax.random.fold_in(arg_keys[12], 71), 0),
        "pred_coords": draw_pred_coords(jax.random.fold_in(arg_keys[12], 71), 0),
        "residue_mask": draw_residue_mask(jax.random.fold_in(arg_keys[12], 71), 0),
        "single": draw_single(jax.random.fold_in(arg_keys[12], 71), 0),
        "ln_gain": jnp.clip(1.0 + 0.18 * jax.random.normal(arg_keys[5], (C_S,), jnp.float32), 0.1, 1.9),
        "w_hidden": normal_values(arg_keys[6], (C_S, HEAD_WIDTH), C_S ** -0.5, 0.3125),
        "b_hidden": normal_values(arg_keys[7], (HEAD_WIDTH,), 0.5, 3.0, jnp.float32),
        "w_mid": normal_values(arg_keys[8], (HEAD_WIDTH, HEAD_WIDTH), HEAD_WIDTH ** -0.5, 0.5),
        "b_mid": normal_values(arg_keys[9], (HEAD_WIDTH,), 0.5, 3.0, jnp.float32),
        "w_logits": normal_values(arg_keys[10], (HEAD_WIDTH, BINS), 0.25, 1.5),
        "b_logits": normal_values(arg_keys[11], (BINS,), 1.0, 4.0, jnp.float32),
    }


THRESHOLDS = (0.5, 1.0, 2.0, 4.0)

def pair_dist(near, far):
    total = (near[0][:, None] - far[0][None, :]) ** 2
    total = total + (near[1][:, None] - far[1][None, :]) ** 2
    total = total + (near[2][:, None] - far[2][None, :]) ** 2
    return jnp.sqrt(total + 1e-10)

def soft_preserved(true_dist, pred_dist):
    mismatch = jnp.abs(pred_dist - true_dist)
    scores = jnp.zeros_like(mismatch)
    for threshold in THRESHOLDS:
        scores = scores + jax.nn.sigmoid(4.0 * (threshold - mismatch))
    return 0.25 * scores

def head_loss(lddt_value, single, ln_gain, w_hidden, b_hidden, w_mid, b_mid, w_logits, b_logits):
    features = single.astype(jnp.float32)
    average = lax.optimization_barrier(jnp.mean(features, axis=-1, keepdims=True))
    centred = features - average
    variance = lax.optimization_barrier(jnp.mean(centred * centred, axis=-1, keepdims=True))
    normed = (centred * lax.rsqrt(variance + 1e-05) * ln_gain).astype(jnp.bfloat16)
    first_hidden = jax.nn.relu(jnp.dot(normed, w_hidden, preferred_element_type=jnp.float32) + b_hidden).astype(jnp.bfloat16)
    second_hidden = jax.nn.relu(jnp.dot(first_hidden, w_mid, preferred_element_type=jnp.float32) + b_mid).astype(jnp.bfloat16)
    logits = jnp.dot(second_hidden, w_logits, preferred_element_type=jnp.float32) + b_logits
    log_total = jnp.log(lax.optimization_barrier(jnp.sum(jnp.exp(logits), axis=-1)))
    bins = logits.shape[-1]
    centers = (jnp.arange(bins).astype(jnp.float32) + 0.5) / bins
    closeness = jnp.exp(-(lddt_value[..., None] - centers) ** 2 * (bins * bins * 0.5))
    target = closeness / lax.optimization_barrier(jnp.sum(closeness, axis=-1, keepdims=True))
    return log_total - lax.optimization_barrier(jnp.sum(target * logits, axis=-1))

def reference(neighbor, true_coords, pred_coords, residue_mask, single, ln_gain, w_hidden, b_hidden, w_mid, b_mid, w_logits, b_logits):
    valid = residue_mask.astype(jnp.float32)

    def per_structure(items):
        contacts, truth, guess, keep = items
        scores = soft_preserved(pair_dist(truth, truth), pair_dist(guess, guess))
        weights = contacts.astype(jnp.float32) * keep[None, :] * keep[:, None]
        return (lax.optimization_barrier(jnp.sum(weights * scores, axis=0)), lax.optimization_barrier(jnp.sum(weights, axis=0)))
    preserved, neighbors = lax.map(per_structure, (neighbor, true_coords, pred_coords, valid))
    lddt_score = preserved / jnp.maximum(neighbors, 1.0)
    residue_loss = valid * head_loss(lddt_score, single, ln_gain, w_hidden, b_hidden, w_mid, b_mid, w_logits, b_logits)
    total_loss = jnp.sum(residue_loss) / jnp.sum(valid)
    return (lddt_score, residue_loss, total_loss)
```

```python
import functools

import jax
import jax.numpy as jnp
from jax import lax
from jax.experimental import pallas as pl
from jax.experimental.pallas import tpu as pltpu
from jax.sharding import PartitionSpec as P

THRESHOLDS = (0.5, 1.0, 2.0, 4.0)
EPS = 1e-10
MESH = pl.DeviceIdType.MESH


def gather_kernel(R, C, x_ref, rows_ref, cols_ref, send_sem, recv_sem, csend_sem, crecv_sem):
    r = lax.axis_index("row")
    c = lax.axis_index("col")
    g = r * C + c
    to_col = g // R
    slot = g % R
    own = to_col == c

    barrier = pltpu.get_barrier_semaphore()
    for k in range(1, C):
        pl.semaphore_signal(barrier, inc=1, device_id=(r, (c + k) % C), device_id_type=MESH)
    for s in range(R):
        source = R * c + s

        @pl.when(source != g)
        def _():
            pl.semaphore_signal(barrier, inc=1, device_id=(source // C, source % C), device_id_type=MESH)

    pl.semaphore_wait(barrier, C - 1 + R - jnp.where(own, 1, 0))

    col_copies = []
    for k in range(1, R):
        copy = pltpu.make_async_remote_copy(
            src_ref=x_ref,
            dst_ref=cols_ref.at[slot],
            send_sem=csend_sem.at[k],
            recv_sem=crecv_sem.at[slot],
            device_id=((r + k) % R, to_col),
            device_id_type=MESH,
        )
        copy.start()
        col_copies.append(copy)
    home = pltpu.make_async_remote_copy(
        src_ref=x_ref,
        dst_ref=cols_ref.at[slot],
        send_sem=csend_sem.at[0],
        recv_sem=crecv_sem.at[slot],
        device_id=(r, to_col),
        device_id_type=MESH,
    )

    @pl.when(jnp.logical_not(own))
    def _():
        home.start()

    row_copies = []
    for k in range(1, C):
        copy = pltpu.make_async_remote_copy(
            src_ref=x_ref,
            dst_ref=rows_ref.at[c],
            send_sem=send_sem.at[k],
            recv_sem=recv_sem.at[k],
            device_id=(r, (c + k) % C),
            device_id_type=MESH,
        )
        copy.start()
        row_copies.append(copy)

    rows_ref[c] = x_ref[...]

    @pl.when(own)
    def _():
        cols_ref[slot] = x_ref[...]

    for copy in row_copies:
        copy.wait()
    for copy in col_copies:
        copy.wait_send()

    @pl.when(jnp.logical_not(own))
    def _():
        home.wait_send()

    for s in range(R):

        @pl.when(R * c + s != g)
        def _():
            pltpu.make_async_remote_copy(
                src_ref=x_ref,
                dst_ref=cols_ref.at[s],
                send_sem=csend_sem.at[0],
                recv_sem=crecv_sem.at[s],
                device_id=(r, to_col),
                device_id_type=MESH,
            ).wait_recv()


def gather(x, R, C):
    shape = x.shape
    return pl.pallas_call(
        functools.partial(gather_kernel, R, C),
        out_shape=(
            jax.ShapeDtypeStruct((C,) + shape, x.dtype),
            jax.ShapeDtypeStruct((R,) + shape, x.dtype),
        ),
        in_specs=[pl.BlockSpec(memory_space=pltpu.VMEM)],
        out_specs=[pl.BlockSpec(memory_space=pltpu.VMEM)] * 2,
        scratch_shapes=[
            pltpu.SemaphoreType.DMA((C,)),
            pltpu.SemaphoreType.DMA((C,)),
            pltpu.SemaphoreType.DMA((R,)),
            pltpu.SemaphoreType.DMA((R,)),
        ],
        compiler_params=pltpu.CompilerParams(collective_id=0, has_side_effects=True),
        name="gather",
    )(x)


def split3(x):
    first = x.astype(jnp.bfloat16).astype(jnp.float32)
    rest = x - first
    second = rest.astype(jnp.bfloat16).astype(jnp.float32)
    return first, second, rest - second


def with_norms(x, row):
    square = x * x
    true_norm = square[0:1] + square[1:2] + square[2:3]
    pred_norm = square[3:4] + square[4:5] + square[5:6]
    mixed = jnp.where(row < 6, x, jnp.where(row == 6, true_norm, pred_norm))
    return mixed, true_norm, pred_norm


def pair_kernel(
    R, C, chunk,
    rows_ref, cols_ref, neighbor_ref, single_ref, gain_ref, wh_ref, bh_ref, wm_ref, bm_ref, wl_ref, bl_ref,
    parts_ref, logits_ref, total_ref,
    left_t, left_p, right, d_true, d_pred, acc_p, acc_n,
):
    b = pl.program_id(0)
    batch = pl.num_programs(0)
    own_len = rows_ref.shape[3]
    rows_len = C * own_len
    cols_len = R * own_len
    rows = jnp.concatenate([rows_ref[s, b] for s in range(C)], axis=1)
    cols = jnp.concatenate([cols_ref[s, b] for s in range(R)], axis=1)
    keep = cols[6:7]
    center = jnp.sum(cols * keep, axis=1, keepdims=True) / jnp.maximum(jnp.sum(keep, axis=1, keepdims=True), 1.0)
    row_r = lax.broadcasted_iota(jnp.int32, rows.shape, 0)
    row_c = lax.broadcasted_iota(jnp.int32, cols.shape, 0)
    far, _, _ = with_norms((rows - center) * 2.0, row_r)
    near = (cols - center) * 2.0
    _, near_t, near_p = with_norms(near, row_c)
    f1, f2, f3 = split3(far)
    ones = jnp.ones_like(far)
    right[...] = jnp.concatenate([f1, f1, f1, f2, f2, f3, ones, jnp.zeros_like(far)], axis=0).astype(jnp.bfloat16)
    n1, n2, n3 = split3(near)
    zeros = jnp.zeros_like(near)
    for ref, low, norm_row, norm in ((left_t, 0, 6, near_t), (left_p, 3, 7, near_p)):
        inside = (row_c >= low) & (row_c < low + 3)
        l1 = jnp.where(inside, -2.0 * n1, jnp.where(row_c == norm_row, 1.0, 0.0))
        l2 = jnp.where(inside, -2.0 * n2, 0.0)
        l3 = jnp.where(inside, -2.0 * n3, 0.0)
        m1, m2, m3 = split3(norm)
        tail = jnp.where(
            row_c == 0, m1, jnp.where(row_c == 1, m2, jnp.where(row_c == 2, m3, jnp.where(row_c == 3, 4.0 * EPS, 0.0)))
        )
        side = jnp.concatenate([l1, l2, l3, l1, l2, l1, tail, zeros], axis=0)
        ref[...] = jnp.transpose(side).astype(jnp.bfloat16)
    keep_col = jnp.transpose(cols)[:, 6:7]
    width = 256
    step = 16
    for q in range(rows_len // width):
        lanes = slice(q * width, (q + 1) * width)
        half = q % 2
        weights_side = right[:, lanes]
        d_true[half] = jnp.dot(left_t[...], weights_side, preferred_element_type=jnp.float32)
        d_pred[half] = jnp.dot(left_p[...], weights_side, preferred_element_type=jnp.float32)
        total_p = jnp.zeros((8, width), jnp.float32)
        total_n = jnp.zeros((8, width), jnp.float32)
        for j in range(0, cols_len, step):
            span = slice(j, j + step)
            t2 = jnp.maximum(d_true[half, span, :], 4.0 * EPS)
            p2 = jnp.maximum(d_pred[half, span, :], 4.0 * EPS)
            gap = jnp.abs(p2 * lax.rsqrt(p2) - t2 * lax.rsqrt(t2))
            w = neighbor_ref[0, span, lanes].astype(jnp.float32) * keep_col[span]
            score = jnp.tanh(2.0 * THRESHOLDS[0] - gap)
            for threshold in THRESHOLDS[1:]:
                score = score + jnp.tanh(2.0 * threshold - gap)
            score = score * w
            for h in range(0, step, 8):
                total_p = total_p + score[h : h + 8]
                total_n = total_n + w[h : h + 8]
        count = jnp.sum(total_n, axis=0, keepdims=True)
        acc_n[pl.ds(b, 1), lanes] = count
        acc_p[pl.ds(b, 1), lanes] = 0.5 * count + 0.125 * jnp.sum(total_p, axis=0, keepdims=True)

    features = single_ref[0].astype(jnp.float32)
    average = jnp.mean(features, axis=-1, keepdims=True)
    centred = features - average
    variance = jnp.mean(centred * centred, axis=-1, keepdims=True)
    normed = (centred * lax.rsqrt(variance + 1e-05) * gain_ref[...]).astype(jnp.bfloat16)
    first = jnp.maximum(
        jnp.dot(normed, wh_ref[...], preferred_element_type=jnp.float32) + bh_ref[...], 0.0
    ).astype(jnp.bfloat16)
    second = jnp.maximum(
        jnp.dot(first, wm_ref[...], preferred_element_type=jnp.float32) + bm_ref[...], 0.0
    ).astype(jnp.bfloat16)
    logits = (
        lax.dot_general(wl_ref[...], second, (((1,), (1,)), ((), ())), preferred_element_type=jnp.float32)
        + bl_ref[...]
    )
    logits_ref[0] = logits
    total_ref[pl.ds(b, 1), :] = jnp.log(jnp.sum(jnp.exp(logits), axis=0, keepdims=True))

    @pl.when(b == batch - 1)
    def _():
        count = acc_p.shape[0]
        for s in range(C):
            lanes = slice(s * own_len, (s + 1) * own_len)
            parts_ref[s, 0:count, :] = acc_p[:, lanes]
            parts_ref[s, count:, :] = acc_n[:, lanes]


def pairs(rows, cols, neighbor, single, gain, wh, bh, wm, bm, wl, bl, R, C):
    batch, cols_len, rows_len = neighbor.shape
    own_len = rows.shape[3]
    bins = wl.shape[0]
    whole = pl.BlockSpec(memory_space=pltpu.VMEM)
    return pl.pallas_call(
        functools.partial(pair_kernel, R, C, 16),
        grid=(batch,),
        in_specs=[
            whole,
            whole,
            pl.BlockSpec((1, cols_len, rows_len), lambda i: (i, 0, 0)),
            pl.BlockSpec((1,) + single.shape[1:], lambda i: (i, 0, 0)),
        ]
        + [whole] * 7,
        out_specs=[
            pl.BlockSpec((C, 2 * batch, own_len), lambda i: (0, 0, 0)),
            pl.BlockSpec((1, bins, own_len), lambda i: (i, 0, 0)),
            pl.BlockSpec((batch, own_len), lambda i: (0, 0)),
        ],
        out_shape=[
            jax.ShapeDtypeStruct((C, 2 * batch, own_len), jnp.float32),
            jax.ShapeDtypeStruct((batch, bins, own_len), jnp.float32),
            jax.ShapeDtypeStruct((batch, own_len), jnp.float32),
        ],
        scratch_shapes=[
            pltpu.VMEM((cols_len, 64), jnp.bfloat16),
            pltpu.VMEM((cols_len, 64), jnp.bfloat16),
            pltpu.VMEM((64, rows_len), jnp.bfloat16),
            pltpu.VMEM((2, cols_len, 256), jnp.float32),
            pltpu.VMEM((2, cols_len, 256), jnp.float32),
            pltpu.VMEM((batch, rows_len), jnp.float32),
            pltpu.VMEM((batch, rows_len), jnp.float32),
        ],
        compiler_params=pltpu.CompilerParams(dimension_semantics=("arbitrary",)),
        name="pairs",
    )(rows, cols, neighbor, single, gain, wh, bh, wm, bm, wl, bl)


def finish_kernel(
    R, C,
    parts_ref, logits_ref, total_ref, valid_ref,
    lddt_ref, loss_ref, mean_ref,
    landed, tile, mid, tiles_c, tiles_r,
    send_sem, recv_sem, csend_sem, crecv_sem, rsend_sem, rrecv_sem,
):
    r = lax.axis_index("row")
    c = lax.axis_index("col")
    barrier = pltpu.get_barrier_semaphore()
    for k in range(1, C):
        pl.semaphore_signal(barrier, inc=1, device_id=(r, (c + k) % C), device_id_type=MESH)
    for k in range(1, R):
        pl.semaphore_signal(barrier, inc=1, device_id=((r + k) % R, c), device_id_type=MESH)
    pl.semaphore_wait(barrier, C + R - 2)

    copies = []
    for k in range(1, C):
        peer = (c + k) % C
        copy = pltpu.make_async_remote_copy(
            src_ref=parts_ref.at[peer],
            dst_ref=landed.at[k],
            send_sem=send_sem.at[k],
            recv_sem=recv_sem.at[k],
            device_id=(r, peer),
            device_id_type=MESH,
        )
        copy.start()
        copies.append(copy)
    sums = parts_ref[c]
    for copy in copies:
        copy.wait()
    for k in range(1, C):
        sums = sums + landed[k]
    batch = valid_ref.shape[0]
    valid = valid_ref[...]
    lddt = valid * sums[0:batch] / jnp.maximum(valid * sums[batch:], 1.0)
    lddt_ref[...] = lddt
    bins = logits_ref.shape[1]
    logits = logits_ref[...]
    centers = (lax.broadcasted_iota(jnp.int32, logits.shape, 1).astype(jnp.float32) + 0.5) / bins
    apart = lddt[:, None, :] - centers
    closeness = jnp.exp(-(apart * apart) * (bins * bins * 0.5))
    expected = jnp.sum(closeness * logits, axis=1) / jnp.sum(closeness, axis=1)
    loss = valid * (total_ref[...] - expected)
    own_len = valid.shape[1]
    tile[...] = jnp.zeros_like(tile)
    tile[0:1, 0:own_len] = jnp.sum(loss, axis=0, keepdims=True)
    tile[1:2, 0:own_len] = jnp.sum(valid, axis=0, keepdims=True)
    loss_ref[...] = loss

    copies = []
    for k in range(1, C):
        copy = pltpu.make_async_remote_copy(
            src_ref=tile,
            dst_ref=tiles_c.at[c],
            send_sem=csend_sem.at[k],
            recv_sem=crecv_sem.at[k],
            device_id=(r, (c + k) % C),
            device_id_type=MESH,
        )
        copy.start()
        copies.append(copy)
    for copy in copies:
        copy.wait()
    tiles_c[c] = tile[...]
    summed = tiles_c[0]
    for k in range(1, C):
        summed = summed + tiles_c[k]
    mid[...] = summed
    copies = []
    for k in range(1, R):
        copy = pltpu.make_async_remote_copy(
            src_ref=mid,
            dst_ref=tiles_r.at[r],
            send_sem=rsend_sem.at[k],
            recv_sem=rrecv_sem.at[k],
            device_id=((r + k) % R, c),
            device_id_type=MESH,
        )
        copy.start()
        copies.append(copy)
    for copy in copies:
        copy.wait()
    tiles_r[r] = mid[...]
    final = tiles_r[0]
    for k in range(1, R):
        final = final + tiles_r[k]
    both = jnp.sum(final, axis=1, keepdims=True)
    mean_ref[...] = jnp.broadcast_to(both[0:1] / both[1:2], mean_ref.shape)


def finish(parts, logits, total, valid, R, C):
    own = valid.shape
    vmem = pl.BlockSpec(memory_space=pltpu.VMEM)
    return pl.pallas_call(
        functools.partial(finish_kernel, R, C),
        out_shape=(
            jax.ShapeDtypeStruct(own, jnp.float32),
            jax.ShapeDtypeStruct(own, jnp.float32),
            jax.ShapeDtypeStruct((8, 128), jnp.float32),
        ),
        in_specs=[vmem] * 4,
        out_specs=[vmem] * 3,
        scratch_shapes=[
            pltpu.VMEM(parts.shape, jnp.float32),
            pltpu.VMEM((8, 128), jnp.float32),
            pltpu.VMEM((8, 128), jnp.float32),
            pltpu.VMEM((C, 8, 128), jnp.float32),
            pltpu.VMEM((R, 8, 128), jnp.float32),
            pltpu.SemaphoreType.DMA((C,)),
            pltpu.SemaphoreType.DMA((C,)),
            pltpu.SemaphoreType.DMA((C,)),
            pltpu.SemaphoreType.DMA((C,)),
            pltpu.SemaphoreType.DMA((R,)),
            pltpu.SemaphoreType.DMA((R,)),
        ],
        compiler_params=pltpu.CompilerParams(collective_id=1, has_side_effects=True),
        name="finish",
    )(parts, logits, total, valid)


def local(
    R, C,
    neighbor,
    true_coords,
    pred_coords,
    residue_mask,
    single,
    ln_gain,
    w_hidden,
    b_hidden,
    w_mid,
    b_mid,
    w_logits,
    b_logits,
):
    valid = residue_mask.astype(jnp.float32)
    stacked = jnp.concatenate(
        [true_coords, pred_coords, valid[:, None, :], jnp.zeros_like(valid)[:, None, :]], axis=1
    )
    rows, cols = gather(stacked, R, C)
    parts, logits, total = pairs(
        rows,
        cols,
        neighbor,
        single,
        ln_gain[None, :],
        w_hidden,
        b_hidden[None, :],
        w_mid,
        b_mid[None, :],
        w_logits.T,
        b_logits[:, None],
        R,
        C,
    )
    lddt_score, residue_loss, mean = finish(parts, logits, total, valid, R, C)
    return (lddt_score, residue_loss, mean[0, 0])


def solution(mesh):
    R = mesh.shape["row"]
    C = mesh.shape["col"]
    both = P(None, ("row", "col"))
    placed = (
        P(None, "col", "row"),
        P(None, None, ("row", "col")),
        P(None, None, ("row", "col")),
        both,
        P(None, ("row", "col"), None),
        P(),
        P(),
        P(),
        P(),
        P(),
        P(),
        P(),
    )
    return jax.shard_map(
        functools.partial(local, R, C),
        mesh=mesh,
        in_specs=placed,
        out_specs=(both, both, P()),
        check_vma=False,
    )
```
